8 devices in a mesh: third: 2 (over z, y), second: 2 (over x), group: 2 (over core).
Axes of the slice: x: 2, y: 2, z: 1, core: 2. Of those that a mesh axis runs over, the one named last changes fastest.
Arguments:
- x_one: bfloat16 [32768, 1024], P(('third', 'second', 'group'))
- z_one: bfloat16 [32768, 4096], P(('third', 'second', 'group'))
- x_two: bfloat16 [32768, 1024], P(('third', 'second', 'group'))
- z_two: bfloat16 [32768, 4096], P(('third', 'second', 'group'))
- grad_out: bfloat16 [32768, 1024], P(('third', 'second', 'group'))
- w1_in: bfloat16 [1024, 4096], replicated
- w1_out: bfloat16 [4096, 1024], replicated
- w2_in: bfloat16 [1024, 4096], replicated
- w2_out: bfloat16 [4096, 1024], replicated
Outputs:
- output 1: float32 [4096, 1024], replicated
- output 2: float32 [1024, 4096], replicated
- output 3: float32 [4096, 1024], replicated
- output 4: float32 [1024, 4096], replicated
- output 5: bfloat16 [32768, 1024], P(('third', 'second', 'group'))
All inputs are finite; a program needn't handle non-finite values.
Results may differ from the reference program's by a relative error of at most 0.00511536.
Values are sent between devices in bfloat16 or wider.
A program may use at most 1 GiB of HBM per device.

```python
import math
import jax
import jax.numpy as jnp
from jax import lax

D = 1024
FF = 4096
TOKENS = 4096
DEVICES = 8

INV_ROOT_TWO = math.sqrt(0.5)
INV_ROOT_TWO_PI = 1.0 / math.sqrt(2.0 * math.pi)


def gelu_pair(z_pre):
    z_val = z_pre.astype(jnp.float32)
    cdf_val = 0.5 * (1.0 + lax.erf(z_val * INV_ROOT_TWO))
    hidden = (z_val * cdf_val).astype(jnp.bfloat16)
    slope = cdf_val + z_val * jnp.exp(-0.5 * z_val * z_val) * INV_ROOT_TWO_PI
    return hidden, slope


def block_backward(x_in, z_pre, grad_y, w_in, w_out):
    hidden, slope = gelu_pair(z_pre)
    w_out_grad = jnp.dot(hidden.T, grad_y, preferred_element_type=jnp.float32).astype(jnp.bfloat16)
    grad_hidden = jnp.dot(grad_y, w_out.T, preferred_element_type=jnp.float32)
    grad_pre = (grad_hidden * slope).astype(jnp.bfloat16)
    w_in_grad = jnp.dot(x_in.T, grad_pre, preferred_element_type=jnp.float32).astype(jnp.bfloat16)
    grad_x = (grad_y.astype(jnp.float32) + jnp.dot(grad_pre, w_in.T, preferred_element_type=jnp.float32)).astype(jnp.bfloat16)
    return w_out_grad, w_in_grad, grad_x


def setup_inputs(seed: int = 0) -> dict:
    keys = jax.random.split(jax.random.key(seed), 9)
    row_count = DEVICES * TOKENS

    def normal_draw(key_part, shape_in, factor):
        return (jax.random.normal(key_part, shape_in, jnp.float32) * factor).astype(jnp.bfloat16)

    return dict(
        x_one=normal_draw(keys[0], (row_count, D), 1.0),
        z_one=normal_draw(keys[1], (row_count, FF), 1.0),
        x_two=normal_draw(keys[2], (row_count, D), 1.0),
        z_two=normal_draw(keys[3], (row_count, FF), 1.0),
        grad_out=normal_draw(keys[4], (row_count, D), row_count ** -0.25),
        w1_in=normal_draw(keys[5], (D, FF), D ** -0.5),
        w1_out=normal_draw(keys[6], (FF, D), FF ** -0.5),
        w2_in=normal_draw(keys[7], (D, FF), D ** -0.5),
        w2_out=normal_draw(keys[8], (FF, D), FF ** -0.5),
    )


def reference(x_one, z_one, x_two, z_two, grad_out, w1_in, w1_out, w2_in, w2_out):
    def by_device(arr):
        return arr.reshape(DEVICES, TOKENS, arr.shape[-1])

    def device_step(run_sums, batch):
        x_one_dev, z_one_dev, x_two_dev, z_two_dev, grad_dev = batch
        w2o_grad, w2i_grad, dx_two = block_backward(x_two_dev, z_two_dev, grad_dev, w2_in, w2_out)
        w1o_grad, w1i_grad, dx_one = block_backward(x_one_dev, z_one_dev, dx_two, w1_in, w1_out)
        new_sums = tuple(run_sum + grad_part.astype(jnp.float32) for run_sum, grad_part in zip(run_sums, (w2o_grad, w2i_grad, w1o_grad, w1i_grad)))
        return new_sums, dx_one

    zero_sums = (
        jnp.zeros((FF, D), jnp.float32),
        jnp.zeros((D, FF), jnp.float32),
        jnp.zeros((FF, D), jnp.float32),
        jnp.zeros((D, FF), jnp.float32),
    )
    batches = (by_device(x_one), by_device(z_one), by_device(x_two), by_device(z_two), by_device(grad_out))
    total_sums, grad_rows = lax.scan(device_step, zero_sums, batches)
    return (total_sums[0], total_sums[1], total_sums[2], total_sums[3], grad_rows.reshape(DEVICES * TOKENS, D))
```

```python
import functools
import math
import jax
import jax.numpy as jnp
from jax import lax
from jax.experimental import pallas as pl
from jax.experimental.pallas import tpu as pltpu
from jax.sharding import PartitionSpec as P

AXES = ('third', 'second', 'group')
INV_ROOT_TWO = math.sqrt(0.5)
INV_ROOT_TWO_PI = 1.0 / math.sqrt(2.0 * math.pi)
MESH = pl.DeviceIdType.MESH
F32 = jnp.float32
BF16 = jnp.bfloat16
TOK, D, FF = 4096, 1024, 4096
FB = 256
NF = FF // FB
NC = 2 * NF
TM = 256
TN = 256
PART = (FB // 4, D // 4)
COLS = (D, FB)
R1, R2, SD, RS = 5, 4, 4, 8


def kernel(x1, z1, x2, z2, dy, w1i, w1o, w2i, w2o, out_o, out_i, dx_out,
           gbuf, xbuf, acc, zbuf, wobuf, wibuf, wot, wit, ht, dzt,
           slab_a, slab_b, got_a, got_b, part_a, part_b, swp_a, swp_b, sum_a, sum_b,
           gsem, xsem, zsem, wosem, wisem, s1, r1, s2, r2, lsem, s3, r3, sf, rf):
    t, s, g = [lax.axis_index(k) for k in AXES]
    near_axis = (s, t)

    def peer(color, flip_one, flip_two, flip_core):
        ft, fs = (flip_two, flip_one) if color == 0 else (flip_one, flip_two)
        return (1 - t if ft else t, 1 - s if fs else s, 1 - g if flip_core else g)

    slab, got, part = (slab_a, slab_b), (got_a, got_b), (part_a, part_b)
    swp, sums = (swp_a, swp_b), (sum_a, sum_b)

    def quarter_of(color, flip_one, flip_core):
        a = near_axis[color]
        return 2 * (1 - a if flip_one else a) + (1 - g if flip_core else g)

    def slab_rows(color, q):
        return pl.ds(pl.multiple_of(q * PART[color], PART[color]), PART[color])

    def first(c, color, k):
        one, core = ((1, 0), (1, 1), (0, 1))[k]
        return pltpu.make_async_remote_copy(
            src_ref=slab[color].at[c % 2, slab_rows(color, quarter_of(color, one, core))],
            dst_ref=got[color].at[c % R1, k],
            send_sem=s1.at[color, c % 2, k], recv_sem=r1.at[color, c % R1, k],
            device_id=peer(color, one, 0, core), device_id_type=MESH)

    def second(c, color):
        return pltpu.make_async_remote_copy(
            src_ref=part[color].at[c % 2], dst_ref=swp[color].at[c % R2],
            send_sem=s2.at[color, c % 2], recv_sem=r2.at[color, c % R2],
            device_id=peer(color, 0, 1, 0), device_id_type=MESH)

    def region(c, color, q):
        b, f = c // NF, c % NF
        if color == 0:
            row = pl.multiple_of(b * FF + f * FB + q * PART[0], PART[0])
            return out_o.at[pl.ds(row, PART[0])]
        row = pl.multiple_of(b * D + q * PART[1], PART[1])
        return out_i.at[pl.ds(row, PART[1]), pl.ds(pl.multiple_of(f * FB, FB), FB)]

    def local(c, color):
        return pltpu.make_async_copy(sums[color].at[c % SD], region(c, color, quarter_of(color, 0, 0)),
                                     lsem.at[color, c % SD])

    def third(c, color, k):
        return pltpu.make_async_remote_copy(
            src_ref=sums[color].at[c % SD], dst_ref=region(c, color, quarter_of(color, 0, 0)),
            send_sem=s3.at[color, c % SD, k], recv_sem=r3.at[color, c % RS, k],
            device_id=peer(color, 1 - k, 0, k), device_id_type=MESH)

    def forward(c, color):
        there = region(c, color, quarter_of(color, 1, 0))
        return pltpu.make_async_remote_copy(
            src_ref=there, dst_ref=there, send_sem=sf.at[color, c % RS], recv_sem=rf.at[color, c % RS],
            device_id=peer(color, 0, 0, 1), device_id_type=MESH)

    def loads(c, zr, wor, wir):
        f = c % NF
        cols = pl.ds(pl.multiple_of(f * FB, FB), FB)
        k = c % 2
        return (pltpu.make_async_copy(zr.at[:, cols], zbuf.at[k], zsem.at[k]),
                pltpu.make_async_copy(wor.at[cols], wobuf.at[k], wosem.at[k]),
                pltpu.make_async_copy(wir.at[:, cols], wibuf.at[k], wisem.at[k]))

    def start_loads(c):
        @pl.when(c < NF)
        def _():
            for copy in loads(c, z2, w2o, w2i):
                copy.start()

        @pl.when(jnp.logical_and(c >= NF, c < NC))
        def _():
            for copy in loads(c, z1, w1o, w1i):
                copy.start()

    start_loads(0)
    pltpu.make_async_copy(dy, gbuf, gsem).start()
    pltpu.make_async_copy(x2, xbuf, xsem).start()

    barrier = pltpu.get_barrier_semaphore()
    peers = ((0, 1, 0, 0), (0, 1, 0, 1), (1, 1, 0, 0), (1, 1, 0, 1), (0, 0, 0, 1))
    for who in peers:
        pl.semaphore_signal(barrier, inc=1, device_id=peer(*who), device_id_type=MESH)
    pl.semaphore_wait(barrier, len(peers))

    pltpu.make_async_copy(dy, gbuf, gsem).wait()

    def compute(c):
        f = c % NF
        k = c % 2

        @pl.when(c == NF)
        def _():
            pltpu.make_async_copy(x1, xbuf, xsem).start()

        start_loads(c + 1)

        @pl.when(f == 0)
        def _():
            @pl.loop(0, TOK // TM)
            def _(r):
                rows = pl.ds(pl.multiple_of(r * TM, TM), TM)
                acc[rows, :] = gbuf[rows, :].astype(F32)

        for copy in loads(c, z2, w2o, w2i):
            copy.wait()
        wot[...] = wobuf[k].T
        wit[...] = wibuf[k].T

        @pl.loop(0, TOK // TM)
        def _(r):
            rows = pl.ds(pl.multiple_of(r * TM, TM), TM)
            z_val = zbuf[k, rows, :].astype(F32)
            cdf_val = 0.5 * (1.0 + lax.erf(z_val * INV_ROOT_TWO))
            ht[:, rows] = (z_val * cdf_val).astype(BF16).T
            slope = cdf_val + z_val * jnp.exp(-0.5 * z_val * z_val) * INV_ROOT_TWO_PI
            grad_hidden = jnp.dot(gbuf[rows, :], wot[...], preferred_element_type=F32)
            grad_pre = (grad_hidden * slope).astype(BF16)
            dzt[:, rows] = grad_pre.T
            acc[rows, :] += jnp.dot(grad_pre, wit[...], preferred_element_type=F32)

        @pl.when(f == 0)
        def _():
            pltpu.make_async_copy(x2, xbuf, xsem).wait()

        @pl.loop(0, D // TN)
        def _(n):
            cols = pl.ds(pl.multiple_of(n * TN, TN), TN)
            slab_a[k, :, cols] = jnp.dot(ht[...], gbuf[:, cols], preferred_element_type=F32).astype(BF16)
            slab_b[k, cols, :] = jnp.dot(dzt[...], xbuf[:, cols], preferred_element_type=F32).T.astype(BF16)

        @pl.when(f == NF - 1)
        def _():
            @pl.loop(0, TOK // TM)
            def _(r):
                rows = pl.ds(pl.multiple_of(r * TM, TM), TM)
                gbuf[rows, :] = acc[rows, :].astype(BF16)

    @pl.loop(0, NC + 6)
    def _(i):
        @pl.when(i < NC)
        def _():
            compute(i)
            for k in range(3):
                for color in range(2):
                    first(i, color, k).start()

        @pl.when(i == NC - 1)
        def _():
            pltpu.make_async_copy(gbuf, dx_out, gsem).start()

        @pl.when(jnp.logical_and(i >= 1, i < NC + 1))
        def _():
            c = i - 1
            for color in range(2):
                for k in range(3):
                    copy = first(c, color, k)
                    copy.wait_recv()
                    copy.wait_send()
                own = slab[color][c % 2, slab_rows(color, quarter_of(color, 0, 0)), :].astype(F32)
                near, far, pair = [got[color][c % R1, k].astype(F32) for k in range(3)]
                part[color][c % 2] = (own + pair) + (near + far)
                second(c, color).start()

        @pl.when(jnp.logical_and(i >= 2, i < NC + 2))
        def _():
            c = i - 2
            for color in range(2):
                copy = second(c, color)
                copy.wait_recv()
                copy.wait_send()
                sums[color][c % SD] = part[color][c % 2] + swp[color][c % R2]
            for color in range(2):
                for k in range(2):
                    third(c, color, k).start()
                local(c, color).start()

        @pl.when(jnp.logical_and(i >= 4, i < NC + 4))
        def _():
            c = i - 4
            for color in range(2):
                third(c, color, 0).wait_recv()
                forward(c, color).start()

        @pl.when(jnp.logical_and(i >= 5, i < NC + 5))
        def _():
            c = i - 5
            for color in range(2):
                third(c, color, 1).wait_recv()
                third(c, color, 0).wait_send()
                third(c, color, 1).wait_send()
                local(c, color).wait()
                forward(c, color).wait_send()
                forward(c, color).wait_recv()

    pltpu.make_async_copy(gbuf, dx_out, gsem).wait()


def solution(mesh):
    def device_step(x_one, z_one, x_two, z_two, grad_out, w1_in, w1_out, w2_in, w2_out):
        dma = pltpu.SemaphoreType.DMA
        out_o, out_i, dx_one = pl.pallas_call(
            kernel,
            out_shape=(jax.ShapeDtypeStruct((2 * FF, D), F32), jax.ShapeDtypeStruct((2 * D, FF), F32),
                       jax.ShapeDtypeStruct((TOK, D), BF16)),
            in_specs=[pl.BlockSpec(memory_space=pl.ANY)] * 9,
            out_specs=[pl.BlockSpec(memory_space=pl.ANY)] * 3,
            scratch_shapes=[
                pltpu.VMEM((TOK, D), BF16), pltpu.VMEM((TOK, D), BF16), pltpu.VMEM((TOK, D), F32),
                pltpu.VMEM((2, TOK, FB), BF16), pltpu.VMEM((2, FB, D), BF16), pltpu.VMEM((2, D, FB), BF16),
                pltpu.VMEM((D, FB), BF16), pltpu.VMEM((FB, D), BF16),
                pltpu.VMEM((FB, TOK), BF16), pltpu.VMEM((FB, TOK), BF16),
                pltpu.VMEM((2, FB, D), BF16), pltpu.VMEM((2, D, FB), BF16),
                pltpu.VMEM((R1, 3, PART[0], D), BF16), pltpu.VMEM((R1, 3, PART[1], FB), BF16),
                pltpu.VMEM((2, PART[0], D), F32), pltpu.VMEM((2, PART[1], FB), F32),
                pltpu.VMEM((R2, PART[0], D), F32), pltpu.VMEM((R2, PART[1], FB), F32),
                pltpu.VMEM((SD, PART[0], D), F32), pltpu.VMEM((SD, PART[1], FB), F32),
                dma, dma, dma((2,)), dma((2,)), dma((2,)),
                dma((2, 2, 3)), dma((2, R1, 3)), dma((2, 2)), dma((2, R2)),
                dma((2, SD)), dma((2, SD, 2)), dma((2, RS, 2)), dma((2, RS)), dma((2, RS)),
            ],
            compiler_params=pltpu.CompilerParams(collective_id=0, has_side_effects=True,
                                                 vmem_limit_bytes=67043328),
        )(x_one, z_one, x_two, z_two, grad_out, w1_in, w1_out, w2_in, w2_out)
        return out_o[:FF], out_i[:D], out_o[FF:], out_i[D:], dx_one

    row_spec = P(AXES, None)
    repl_spec = P()
    return jax.shard_map(
        device_step,
        mesh=mesh,
        in_specs=(row_spec, row_spec, row_spec, row_spec, row_spec, repl_spec, repl_spec, repl_spec, repl_spec),
        out_specs=(repl_spec, repl_spec, repl_spec, repl_spec, row_spec),
        check_vma=False,
    )
```

```python
import functools
import math
import jax
import jax.numpy as jnp
from jax import lax
from jax.experimental import pallas as pl
from jax.experimental.pallas import tpu as pltpu
from jax.sharding import PartitionSpec as P

AXES = ('third', 'second', 'group')
INV_ROOT_TWO = math.sqrt(0.5)
INV_ROOT_TWO_PI = 1.0 / math.sqrt(2.0 * math.pi)
MESH = pl.DeviceIdType.MESH
F32 = jnp.float32
BF16 = jnp.bfloat16
TOK, D, FF = 4096, 1024, 4096
FB = 256
NF = FF // FB
NC = 2 * NF
TM = 1024
TN = 1024
PART = (FB // 4, D // 4)
COLS = (D, FB)
R1, R2, SD, RS = 5, 4, 4, 8
LATE = 4
NL = NF // LATE


def kernel(x1, z1, x2, z2, dy, w1i, w1o, w2i, w2o, out_o, out_i, dx_out,
           late_a2, late_b2, late_a1, late_b1,
           gbuf, xbuf, acc, zbuf, wobuf, wibuf, wot, wit, ht, dzt, dzrow,
           slab_a, slab_b, got_a, got_b, part_a, part_b, swp_a, swp_b, sum_a, sum_b,
           gsem, xsem, zsem, wosem, wisem, s1, r1, s2, r2, lsem, s3, r3, sf, rf):
    t, s, g = [lax.axis_index(k) for k in AXES]
    near_axis = (s, t)

    def peer(color, flip_one, flip_two, flip_core):
        ft, fs = (flip_two, flip_one) if color == 0 else (flip_one, flip_two)
        return (1 - t if ft else t, 1 - s if fs else s, 1 - g if flip_core else g)

    slab, got, part = (slab_a, slab_b), (got_a, got_b), (part_a, part_b)
    swp, sums = (swp_a, swp_b), (sum_a, sum_b)

    def quarter_of(color, flip_one, flip_core):
        a = near_axis[color]
        return 2 * (1 - a if flip_one else a) + (1 - g if flip_core else g)

    def slab_rows(color, q):
        return pl.ds(pl.multiple_of(q * PART[color], PART[color]), PART[color])

    def first(c, color, k):
        one, core = ((1, 0), (1, 1), (0, 1))[k]
        return pltpu.make_async_remote_copy(
            src_ref=slab[color].at[c % 2, slab_rows(color, quarter_of(color, one, core))],
            dst_ref=got[color].at[c % R1, k],
            send_sem=s1.at[color, c % 2, k], recv_sem=r1.at[color, c % R1, k],
            device_id=peer(color, one, 0, core), device_id_type=MESH)

    def second(c, color):
        return pltpu.make_async_remote_copy(
            src_ref=part[color].at[c % 2], dst_ref=swp[color].at[c % R2],
            send_sem=s2.at[color, c % 2], recv_sem=r2.at[color, c % R2],
            device_id=peer(color, 0, 1, 0), device_id_type=MESH)

    def region(c, color, q):
        b, f = c // NF, c % NF
        if color == 0:
            row = pl.multiple_of(b * FF + f * FB + q * PART[0], PART[0])
            return out_o.at[pl.ds(row, PART[0])]
        row = pl.multiple_of(b * D + q * PART[1], PART[1])
        return out_i.at[pl.ds(row, PART[1]), pl.ds(pl.multiple_of(f * FB, FB), FB)]

    def local(c, color):
        return pltpu.make_async_copy(sums[color].at[c % SD], region(c, color, quarter_of(color, 0, 0)),
                                     lsem.at[color, c % SD])

    def late_local(c, color, block):
        dst = ((late_a2, late_b2), (late_a1, late_b1))[block][color]
        return pltpu.make_async_copy(sums[color].at[c % SD], dst.at[(c % NF) // LATE], lsem.at[color, c % SD])

    def third(c, color, k):
        return pltpu.make_async_remote_copy(
            src_ref=sums[color].at[c % SD], dst_ref=region(c, color, quarter_of(color, 0, 0)),
            send_sem=s3.at[color, c % SD, k], recv_sem=r3.at[color, c % RS, k],
            device_id=peer(color, 1 - k, 0, k), device_id_type=MESH)

    def forward(c, color):
        there = region(c, color, quarter_of(color, 1, 0))
        return pltpu.make_async_remote_copy(
            src_ref=there, dst_ref=there, send_sem=sf.at[color, c % RS], recv_sem=rf.at[color, c % RS],
            device_id=peer(color, 0, 0, 1), device_id_type=MESH)

    def loads(c, zr, wor, wir):
        f = c % NF
        cols = pl.ds(pl.multiple_of(f * FB, FB), FB)
        k = c % 2
        return (pltpu.make_async_copy(zr.at[:, cols], zbuf.at[k], zsem.at[k]),
                pltpu.make_async_copy(wor.at[cols], wobuf.at[k], wosem.at[k]),
                pltpu.make_async_copy(wir.at[:, cols], wibuf.at[k], wisem.at[k]))

    def start_loads(c):
        @pl.when(c < NF)
        def _():
            for copy in loads(c, z2, w2o, w2i):
                copy.start()

        @pl.when(jnp.logical_and(c >= NF, c < NC))
        def _():
            for copy in loads(c, z1, w1o, w1i):
                copy.start()

    start_loads(0)
    pltpu.make_async_copy(dy, gbuf, gsem).start()
    pltpu.make_async_copy(x2, xbuf, xsem).start()

    barrier = pltpu.get_barrier_semaphore()
    peers = ((0, 1, 0, 0), (0, 1, 0, 1), (1, 1, 0, 0), (1, 1, 0, 1), (0, 0, 0, 1))
    for who in peers:
        pl.semaphore_signal(barrier, inc=1, device_id=peer(*who), device_id_type=MESH)
    pl.semaphore_wait(barrier, len(peers))

    pltpu.make_async_copy(dy, gbuf, gsem).wait()

    def compute(c):
        f = c % NF
        k = c % 2

        @pl.when(c == NF)
        def _():
            pltpu.make_async_copy(x1, xbuf, xsem).start()

        start_loads(c + 1)

        @pl.when(f == 0)
        def _():
            @pl.loop(0, TOK // TM)
            def _(r):
                rows = pl.ds(pl.multiple_of(r * TM, TM), TM)
                acc[rows, :] = gbuf[rows, :].astype(F32)

        for copy in loads(c, z2, w2o, w2i):
            copy.wait()
        wot[...] = wobuf[k].T
        wit[...] = wibuf[k].T

        def grad_tile(r):
            rows = pl.ds(pl.multiple_of(r * TM, TM), TM)
            z_val = zbuf[k, rows, :].astype(F32)
            cdf_val = 0.5 * (1.0 + lax.erf(z_val * INV_ROOT_TWO))
            ht[:, rows] = (z_val * cdf_val).astype(BF16).T
            slope = cdf_val + z_val * jnp.exp(-0.5 * z_val * z_val) * INV_ROOT_TWO_PI
            grad_hidden = jnp.dot(gbuf[rows, :], wot[...], preferred_element_type=F32)
            grad_pre = (grad_hidden * slope).astype(BF16)
            dzt[:, rows] = grad_pre.T
            dzrow[r % 2] = grad_pre

        def add_tile(r):
            rows = pl.ds(pl.multiple_of(r * TM, TM), TM)
            acc[rows, :] += jnp.dot(dzrow[r % 2], wit[...], preferred_element_type=F32)

        grad_tile(0)

        @pl.loop(1, TOK // TM)
        def _(r):
            add_tile(r - 1)
            grad_tile(r)

        add_tile(TOK // TM - 1)

        @pl.when(f == 0)
        def _():
            pltpu.make_async_copy(x2, xbuf, xsem).wait()

        @pl.loop(0, D // TN)
        def _(n):
            cols = pl.ds(pl.multiple_of(n * TN, TN), TN)
            slab_a[k, :, cols] = jnp.dot(ht[...], gbuf[:, cols], preferred_element_type=F32).astype(BF16)
            slab_b[k, cols, :] = jnp.dot(dzt[...], xbuf[:, cols], preferred_element_type=F32).T.astype(BF16)

        @pl.when(f == NF - 1)
        def _():
            @pl.loop(0, TOK // TM)
            def _(r):
                rows = pl.ds(pl.multiple_of(r * TM, TM), TM)
                gbuf[rows, :] = acc[rows, :].astype(BF16)

    @pl.loop(0, NC + 6)
    def _(i):
        @pl.when(i < NC)
        def _():
            compute(i)
            for k in range(3):
                for color in range(2):
                    first(i, color, k).start()

        @pl.when(i == NC - 1)
        def _():
            pltpu.make_async_copy(gbuf, dx_out, gsem).start()

        @pl.when(jnp.logical_and(i >= 1, i < NC + 1))
        def _():
            c = i - 1
            for color in range(2):
                for k in range(3):
                    copy = first(c, color, k)
                    copy.wait_recv()
                    copy.wait_send()
                own = slab[color][c % 2, slab_rows(color, quarter_of(color, 0, 0)), :].astype(F32)
                near, far, pair = [got[color][c % R1, k].astype(F32) for k in range(3)]
                part[color][c % 2] = (own + pair) + (near + far)
                second(c, color).start()

        @pl.when(jnp.logical_and(i >= 2, i < NC + 2))
        def _():
            c = i - 2
            for color in range(2):
                copy = second(c, color)
                copy.wait_recv()
                copy.wait_send()
                sums[color][c % SD] = part[color][c % 2] + swp[color][c % R2]
            late = c % LATE == LATE - 1

            @pl.when(jnp.logical_not(late))
            def _():
                for color in range(2):
                    for k in range(2):
                        third(c, color, k).start()
                    local(c, color).start()

            @pl.when(jnp.logical_and(late, c < NF))
            def _():
                for color in range(2):
                    late_local(c, color, 0).start()

            @pl.when(jnp.logical_and(late, c >= NF))
            def _():
                for color in range(2):
                    late_local(c, color, 1).start()

        @pl.when(jnp.logical_and(jnp.logical_and(i >= 4, i < NC + 4), (i - 4) % LATE != LATE - 1))
        def _():
            c = i - 4
            for color in range(2):
                third(c, color, 0).wait_recv()
                forward(c, color).start()

        @pl.when(jnp.logical_and(i >= 5, i < NC + 5))
        def _():
            c = i - 5
            for color in range(2):
                late_local(c, color, 0).wait()

            @pl.when(c % LATE != LATE - 1)
            def _():
                for color in range(2):
                    third(c, color, 1).wait_recv()
                    third(c, color, 0).wait_send()
                    third(c, color, 1).wait_send()
                    forward(c, color).wait_send()
                    forward(c, color).wait_recv()

    pltpu.make_async_copy(gbuf, dx_out, gsem).wait()


def swap(value, third=0, second=0, group=0):
    pairs = []
    for t in range(2):
        for s in range(2):
            for g in range(2):
                pairs.append((t * 4 + s * 2 + g, (t ^ third) * 4 + (s ^ second) * 2 + (g ^ group)))
    return lax.ppermute(value, AXES, pairs)


def late_region(ref, color, m, q):
    f = m * LATE + LATE - 1
    if color == 0:
        return ref.at[pl.ds(pl.multiple_of(f * FB + q * PART[0], PART[0]), PART[0])]
    return ref.at[pl.ds(pl.multiple_of(q * PART[1], PART[1]), PART[1]), pl.ds(f * FB, FB)]


def my_quarter(color, flip_one, flip_core):
    a = lax.axis_index(('second', 'third')[color])
    g = lax.axis_index('group')
    return 2 * (1 - a if flip_one else a) + (1 - g if flip_core else g)


CB, CL = 6, 3


def copy_kernel(out_o, out_i, dx_tmp, late_a2, late_b2, late_a1, late_b1,
                w2o, w2i, w1o, w1i, dx, buf_a, buf_b, buf_x, buf_la, buf_lb, isem, osem, xsem, ysem, lsem, msem):
    jobs = []
    early = (LATE - 1) * FB
    for b, (wo, wi) in enumerate(((w2o, w2i), (w1o, w1i))):
        for m in range(NL):
            rows = pl.ds(m * LATE * FB, early)
            jobs.append((out_o.at[pl.ds(b * FF + m * LATE * FB, early)], wo.at[rows], buf_a))
            jobs.append((out_i.at[pl.ds(b * D, D), rows], wi.at[:, rows], buf_b))
    ins, outs = [], []
    for j, (src, dst, buf) in enumerate(jobs):
        k = (j // 2) % (CB // 2)
        ins.append(pltpu.make_async_copy(src, buf.at[k], isem.at[j % 2, k]))
        outs.append(pltpu.make_async_copy(buf.at[k], dst, osem.at[j % 2, k]))
    own = []
    for b, (la, lb, wo, wi) in enumerate(((late_a2, late_b2, w2o, w2i), (late_a1, late_b1, w1o, w1i))):
        for color, (src, dst, buf) in enumerate(((la, wo, buf_la), (lb, wi, buf_lb))):
            q = my_quarter(color, 0, 0)
            own.append((pltpu.make_async_copy(src, buf.at[b], lsem.at[b, color]),
                        [pltpu.make_async_copy(buf.at[b, m], late_region(dst, color, m, q), msem.at[b, color, m])
                         for m in range(NL)]))
    x_in = pltpu.make_async_copy(dx_tmp, buf_x, xsem)
    x_out = pltpu.make_async_copy(buf_x, dx, ysem)
    n = len(jobs)
    x_in.start()
    for fetch, _ in own:
        fetch.start()
    for j in range(n + CL):
        if j < n:
            if j >= CB:
                outs[j - CB].wait()
            ins[j].start()
        if j >= CL:
            ins[j - CL].wait()
            outs[j - CL].start()
    x_in.wait()
    x_out.start()
    for fetch, puts in own:
        fetch.wait()
        for put in puts:
            put.start()
    for j in range(n - CB, n):
        outs[j].wait()
    x_out.wait()
    for _, puts in own:
        for put in puts:
            put.wait()


def place_kernel(flips, *refs):
    n = 2 * len(flips)
    blocks, outs, sem = refs[:n], refs[n + 2:n + 4], refs[n + 4]
    copies = []
    for j, (one, core) in enumerate(flips):
        for color in range(2):
            q = my_quarter(color, one, core)
            for m in range(NL):
                copies.append(pltpu.make_async_copy(blocks[2 * j + color].at[m], late_region(outs[color], color, m, q),
                                                    sem.at[j, color, m]))
    for copy in copies:
        copy.start()
    for copy in copies:
        copy.wait()


def place(sum_o, sum_i, flips, blocks):
    n = len(blocks)
    return pl.pallas_call(
        functools.partial(place_kernel, flips),
        out_shape=(jax.ShapeDtypeStruct((FF, D), F32), jax.ShapeDtypeStruct((D, FF), F32)),
        in_specs=[pl.BlockSpec(memory_space=pltpu.VMEM)] * n + [pl.BlockSpec(memory_space=pl.ANY)] * 2,
        out_specs=[pl.BlockSpec(memory_space=pl.ANY)] * 2,
        input_output_aliases={n: 0, n + 1: 1},
        scratch_shapes=[pltpu.SemaphoreType.DMA((len(flips), 2, NL))],
    )(*blocks, sum_o, sum_i)


def solution(mesh):
    def device_step(x_one, z_one, x_two, z_two, grad_out, w1_in, w1_out, w2_in, w2_out):
        dma = pltpu.SemaphoreType.DMA
        late_a = jax.ShapeDtypeStruct((NL, PART[0], D), F32)
        late_b = jax.ShapeDtypeStruct((NL, PART[1], FB), F32)
        out_o, out_i, dx_tmp, a2, b2, a1, b1 = pl.pallas_call(
            kernel,
            out_shape=(jax.ShapeDtypeStruct((2 * FF, D), F32), jax.ShapeDtypeStruct((2 * D, FF), F32),
                       jax.ShapeDtypeStruct((TOK, D), BF16),
                       late_a, late_b, late_a, late_b),
            in_specs=[pl.BlockSpec(memory_space=pl.ANY)] * 9,
            out_specs=[pl.BlockSpec(memory_space=pl.ANY)] * 7,
            scratch_shapes=[
                pltpu.VMEM((TOK, D), BF16), pltpu.VMEM((TOK, D), BF16), pltpu.VMEM((TOK, D), F32),
                pltpu.VMEM((2, TOK, FB), BF16), pltpu.VMEM((2, FB, D), BF16), pltpu.VMEM((2, D, FB), BF16),
                pltpu.VMEM((D, FB), BF16), pltpu.VMEM((FB, D), BF16),
                pltpu.VMEM((FB, TOK), BF16), pltpu.VMEM((FB, TOK), BF16), pltpu.VMEM((2, TM, FB), BF16),
                pltpu.VMEM((2, FB, D), BF16), pltpu.VMEM((2, D, FB), BF16),
                pltpu.VMEM((R1, 3, PART[0], D), BF16), pltpu.VMEM((R1, 3, PART[1], FB), BF16),
                pltpu.VMEM((2, PART[0], D), F32), pltpu.VMEM((2, PART[1], FB), F32),
                pltpu.VMEM((R2, PART[0], D), F32), pltpu.VMEM((R2, PART[1], FB), F32),
                pltpu.VMEM((SD, PART[0], D), F32), pltpu.VMEM((SD, PART[1], FB), F32),
                dma, dma, dma((2,)), dma((2,)), dma((2,)),
                dma((2, 2, 3)), dma((2, R1, 3)), dma((2, 2)), dma((2, R2)),
                dma((2, SD)), dma((2, SD, 2)), dma((2, RS, 2)), dma((2, RS)), dma((2, RS)),
            ],
            compiler_params=pltpu.CompilerParams(collective_id=0, has_side_effects=True,
                                                 vmem_limit_bytes=67043328),
        )(x_one, z_one, x_two, z_two, grad_out, w1_in, w1_out, w2_in, w2_out)
        xa2, xb2 = swap(a2, second=1), swap(b2, third=1)
        xa1, xb1 = swap(a1, second=1), swap(b1, third=1)
        pa2, pb2, pa1, pb1 = [swap(v, group=1) for v in (a2, b2, a1, b1)]
        flat_o = jax.ShapeDtypeStruct((FF, D), F32)
        flat_i = jax.ShapeDtypeStruct((D, FF), F32)
        early = (LATE - 1) * FB
        w2o, w2i, w1o, w1i, dx_one = pl.pallas_call(
            copy_kernel,
            out_shape=(flat_o, flat_i, flat_o, flat_i, jax.ShapeDtypeStruct((TOK, D), BF16)),
            in_specs=[pl.BlockSpec(memory_space=pl.ANY)] * 7,
            out_specs=[pl.BlockSpec(memory_space=pl.ANY)] * 5,
            scratch_shapes=[
                pltpu.VMEM((CB // 2, early, D), F32), pltpu.VMEM((CB // 2, D, early), F32),
                pltpu.VMEM((TOK, D), BF16), pltpu.VMEM((2, NL, PART[0], D), F32), pltpu.VMEM((2, NL, PART[1], FB), F32),
                dma((2, CB // 2)), dma((2, CB // 2)), dma, dma, dma((2, 2)), dma((2, 2, NL)),
            ],
            compiler_params=pltpu.CompilerParams(vmem_limit_bytes=50 * 2 ** 20),
            cost_estimate=pl.CostEstimate(flops=4 * 10 ** 8, bytes_accessed=150 * 10 ** 6, transcendentals=0),
        )(out_o, out_i, dx_tmp, a2, b2, a1, b1)
        w2o, w2i, w1o, w1i, xa2, xb2, xa1, xb1 = lax.optimization_barrier((w2o, w2i, w1o, w1i, xa2, xb2, xa1, xb1))
        fa2, fb2, fa1, fb1 = [swap(v, group=1) for v in (xa2, xb2, xa1, xb1)]
        w2o, w2i = place(w2o, w2i, ((0, 1), (1, 0), (1, 1)), (pa2, pb2, xa2, xb2, fa2, fb2))
        w1o, w1i = place(w1o, w1i, ((0, 1),), (pa1, pb1))
        w1o, w1i = place(w1o, w1i, ((1, 0), (1, 1)), (xa1, xb1, fa1, fb1))
        return w2o, w2i, w1o, w1i, dx_one

    row_spec = P(AXES, None)
    repl_spec = P()
    return jax.shard_map(
        device_step,
        mesh=mesh,
        in_specs=(row_spec, row_spec, row_spec, row_spec, row_spec, repl_spec, repl_spec, repl_spec, repl_spec),
        out_specs=(repl_spec, repl_spec, repl_spec, repl_spec, row_spec),
        check_vma=False,
    )
```

```python
import functools
import math
import jax
import jax.numpy as jnp
from jax import lax
from jax.experimental import pallas as pl
from jax.experimental.pallas import tpu as pltpu
from jax.sharding import PartitionSpec as P

AXES = ('third', 'second', 'group')
INV_ROOT_TWO = math.sqrt(0.5)
INV_ROOT_TWO_PI = 1.0 / math.sqrt(2.0 * math.pi)
MESH = pl.DeviceIdType.MESH
F32 = jnp.float32
BF16 = jnp.bfloat16
TOK, D, FF = 4096, 1024, 4096
FB = 256
NF = FF // FB
NC = 2 * NF
TM = 1024
PART = (FB // 4, D // 4)
COLS = (D, FB)
LB, LC, LD, LE = 1, 2, 4, 5
NS, NP = LB + 1, LC - LB + 1
R1, R2, SD, RS = 2 * LB + 3, 2 * (LC - LB) + 2, LE - LC + 1, 12
GROUPS = (((0, 3), (0, 7), (0, 11), (0, 15)), ((1, 3), (1, 5), (1, 7), (1, 9)), ((1, 11), (1, 14), (1, 15)))
RUNS = (((0, 3), (4, 3), (8, 3), (12, 3)),
        ((0, 3), (4, 1), (6, 1), (8, 1), (10, 1), (12, 2)))
PIECES = 4


def kernel(x1, z1, x2, z2, dy, w1i, w1o, w2i, w2o, out_o, out_i, dx_out,
           *rest):
    (late_a0, late_b0, late_a1, late_b1, late_a2, late_b2,
           gbuf, xbuf, acc, zbuf, wobuf, wibuf, wot, wit, ht, dzt, dzrow,
           slab_a, slab_b, got_a, got_b, part_a, part_b, swp_a, swp_b, sum_a, sum_b,
           gsem, xsem, zsem, wosem, wisem, s1, r1, s2, r2, lsem, s3, r3, sf, rf) = rest
    t, s, g = [lax.axis_index(k) for k in AXES]
    near_axis = (s, t)

    def peer(color, flip_one, flip_two, flip_core):
        ft, fs = (flip_two, flip_one) if color == 0 else (flip_one, flip_two)
        return (1 - t if ft else t, 1 - s if fs else s, 1 - g if flip_core else g)

    slab, got, part = (slab_a, slab_b), (got_a, got_b), (part_a, part_b)
    swp, sums = (swp_a, swp_b), (sum_a, sum_b)

    def quarter_of(color, flip_one, flip_core):
        a = near_axis[color]
        return 2 * (1 - a if flip_one else a) + (1 - g if flip_core else g)

    def slab_rows(color, q):
        return pl.ds(pl.multiple_of(q * PART[color], PART[color]), PART[color])

    def first(c, color, k):
        one, core = ((1, 0), (1, 1), (0, 1))[k]
        return pltpu.make_async_remote_copy(
            src_ref=slab[color].at[c % NS, slab_rows(color, quarter_of(color, one, core))],
            dst_ref=got[color].at[c % R1, k],
            send_sem=s1.at[color, c % NS, k], recv_sem=r1.at[color, c % R1, k],
            device_id=peer(color, one, 0, core), device_id_type=MESH)

    def second(c, color):
        return pltpu.make_async_remote_copy(
            src_ref=part[color].at[c % NP], dst_ref=swp[color].at[c % R2],
            send_sem=s2.at[color, c % NP], recv_sem=r2.at[color, c % R2],
            device_id=peer(color, 0, 1, 0), device_id_type=MESH)

    def region(c, color, q):
        b, f = c // NF, c % NF
        if color == 0:
            row = pl.multiple_of(b * FF + f * FB + q * PART[0], PART[0])
            return out_o.at[pl.ds(row, PART[0])]
        row = pl.multiple_of(b * D + q * PART[1], PART[1])
        return out_i.at[pl.ds(row, PART[1]), pl.ds(pl.multiple_of(f * FB, FB), FB)]

    def local(c, color):
        return pltpu.make_async_copy(sums[color].at[c % SD], region(c, color, quarter_of(color, 0, 0)),
                                     lsem.at[color, c % SD])

    lates = ((late_a0, late_b0), (late_a1, late_b1), (late_a2, late_b2))

    def is_late(c):
        odd = jnp.logical_and(c % 2 == 1, jnp.logical_or(c % 4 == 3, c >= NF + 4))
        return jnp.logical_and(jnp.logical_or(odd, c == NC - 2), c != NC - 3)

    def late_local(c, color, group):
        index = (c // 4, (c - NF - 3) // 2, jnp.where(c >= NC - 2, c - (NC - 3), 0))[group]
        return pltpu.make_async_copy(sums[color].at[c % SD], lates[group][color].at[index], lsem.at[color, SD + c % SD])

    def in_group(c, group):
        low, high = ((0, NF), (NF, NF + 10), (NF + 10, NC))[group]
        return jnp.logical_and(is_late(c), jnp.logical_and(c >= low, c < high))

    def third(c, color, k):
        return pltpu.make_async_remote_copy(
            src_ref=sums[color].at[c % SD], dst_ref=region(c, color, quarter_of(color, 0, 0)),
            send_sem=s3.at[color, c % SD, k], recv_sem=r3.at[color, c % RS, k],
            device_id=peer(color, 1 - k, 0, k), device_id_type=MESH)

    def forward(c, color):
        there = region(c, color, quarter_of(color, 1, 0))
        return pltpu.make_async_remote_copy(
            src_ref=there, dst_ref=there, send_sem=sf.at[color, c % RS], recv_sem=rf.at[color, c % RS],
            device_id=peer(color, 0, 0, 1), device_id_type=MESH)

    def loads(c, zr, wor, wir):
        f = c % NF
        cols = pl.ds(pl.multiple_of(f * FB, FB), FB)
        k = c % 2
        return (pltpu.make_async_copy(zr.at[:, cols], zbuf.at[k], zsem.at[k]),
                pltpu.make_async_copy(wor.at[cols], wobuf.at[k], wosem.at[k]),
                pltpu.make_async_copy(wir.at[:, cols], wibuf.at[k], wisem.at[k]))

    def start_loads(c):
        @pl.when(c < NF)
        def _():
            for copy in loads(c, z2, w2o, w2i):
                copy.start()

        @pl.when(jnp.logical_and(c >= NF, c < NC))
        def _():
            for copy in loads(c, z1, w1o, w1i):
                copy.start()

    start_loads(0)
    def first_rows(j):
        rows = pl.ds(j * (TOK // PIECES), TOK // PIECES)
        return pltpu.make_async_copy(dy.at[rows], gbuf.at[rows], gsem.at[j])

    for j in range(PIECES):
        first_rows(j).start()

    barrier = pltpu.get_barrier_semaphore()
    peers = ((0, 1, 0, 0), (0, 1, 0, 1), (1, 1, 0, 0), (1, 1, 0, 1), (0, 0, 0, 1))
    for who in peers:
        pl.semaphore_signal(barrier, inc=1, device_id=peer(*who), device_id_type=MESH)
    pl.semaphore_wait(barrier, len(peers))

    pltpu.make_async_copy(x2, xbuf, xsem).start()
    first_rows(0).wait()

    def compute_hidden(c):
        f = c % NF
        k = c % 2

        @pl.when(c == NF)
        def _():
            pltpu.make_async_copy(x1, xbuf, xsem).start()

        start_loads(c + 1)

        for copy in loads(c, z2, w2o, w2i):
            copy.wait()
        wot[...] = wobuf[k].T
        wit[...] = wibuf[k].T

        def grad_tile(r):
            rows = pl.ds(pl.multiple_of(r * TM, TM), TM)
            z_val = zbuf[k, rows, :].astype(F32)
            cdf_val = 0.5 * (1.0 + lax.erf(z_val * INV_ROOT_TWO))
            ht[:, rows] = (z_val * cdf_val).astype(BF16).T
            slope = cdf_val + z_val * jnp.exp(-0.5 * z_val * z_val) * INV_ROOT_TWO_PI
            grad_hidden = jnp.dot(gbuf[rows, :], wot[...], preferred_element_type=F32)
            grad_pre = (grad_hidden * slope).astype(BF16)
            dzt[:, rows] = grad_pre.T
            dzrow[r % 2] = grad_pre

        def add_tile(r, base):
            rows = pl.ds(pl.multiple_of(r * TM, TM), TM)
            acc[rows, :] = base[rows, :].astype(F32) + jnp.dot(dzrow[r % 2], wit[...], preferred_element_type=F32)

        def hidden_phase(base, before_rest):
            grad_tile(0)
            before_rest()

            @pl.loop(1, TOK // TM)
            def _(r):
                add_tile(r - 1, base)
                grad_tile(r)

            add_tile(TOK // TM - 1, base)

        @pl.when(f == 0)
        def _():
            def before_rest():
                @pl.when(c == 0)
                def _():
                    for j in range(1, PIECES):
                        first_rows(j).wait()

            hidden_phase(gbuf, before_rest)

        @pl.when(f > 0)
        def _():
            hidden_phase(acc, lambda: None)

    def compute_weights(c):
        f = c % NF
        slab_a[c % NS] = jnp.dot(ht[...], gbuf[...], preferred_element_type=F32).astype(BF16)
        for j in range(3):
            first(c, 0, j).start()

        @pl.when(f == 0)
        def _():
            pltpu.make_async_copy(x2, xbuf, xsem).wait()

        slab_b[c % NS] = jnp.dot(dzt[...], xbuf[...], preferred_element_type=F32).T.astype(BF16)
        for j in range(3):
            first(c, 1, j).start()

        @pl.when(f == NF - 1)
        def _():
            @pl.loop(0, TOK // TM)
            def _(r):
                rows = pl.ds(pl.multiple_of(r * TM, TM), TM)
                gbuf[rows, :] = acc[rows, :].astype(BF16)

    def add_first(c):
        for color in range(2):
            for k in range(3):
                copy = first(c, color, k)
                copy.wait_recv()
                copy.wait_send()
            own = slab[color][c % NS, slab_rows(color, quarter_of(color, 0, 0)), :].astype(F32)
            near, far, pair = [got[color][c % R1, k].astype(F32) for k in range(3)]
            part[color][c % NP] = (own + pair) + (near + far)
            second(c, color).start()

    @pl.loop(0, NC + LE)
    def _(i):
        @pl.when(i < NC)
        def _():
            compute_hidden(i)

        @pl.when(i == 1)
        def _():
            add_first(0)

        @pl.when(i < NC)
        def _():
            compute_weights(i)

        @pl.when(i == NC - 1)
        def _():
            pltpu.make_async_copy(gbuf, dx_out, gsem.at[0]).start()

        @pl.when(jnp.logical_and(i >= 2, i < NC + LB))
        def _():
            add_first(i - LB)

        @pl.when(jnp.logical_and(jnp.logical_and(i >= 1, i != 2), i < NC + LC))
        def _():
            c = jnp.where(i == 1, 0, i - LC)
            for color in range(2):
                copy = second(c, color)
                copy.wait_recv()
                copy.wait_send()
                sums[color][c % SD] = part[color][c % NP] + swp[color][c % R2]
            for color in range(2):
                third(c, color, 1).start()
                local(c, color).start()

            @pl.when(jnp.logical_not(is_late(c)))
            def _():
                for color in range(2):
                    third(c, color, 0).start()

            for group in range(len(GROUPS)):
                @pl.when(in_group(c, group))
                def _():
                    for color in range(2):
                        late_local(c, color, group).start()

        @pl.when(jnp.logical_and(jnp.logical_and(i >= LD, i < NC + LD), jnp.logical_not(is_late(i - LD))))
        def _():
            c = i - LD
            for color in range(2):
                third(c, color, 0).wait_recv()
                forward(c, color).start()

        @pl.when(jnp.logical_and(i >= LE, i < NC + LE))
        def _():
            c = i - LE
            for color in range(2):
                third(c, color, 1).wait_recv()
                third(c, color, 1).wait_send()
                local(c, color).wait()

            @pl.when(is_late(c))
            def _():
                for color in range(2):
                    pltpu.make_async_copy(sums[color].at[c % SD], lates[0][color].at[0],
                                          lsem.at[color, SD + c % SD]).wait()

            @pl.when(jnp.logical_not(is_late(c)))
            def _():
                for color in range(2):
                    third(c, color, 0).wait_send()
                    forward(c, color).wait_send()
                    forward(c, color).wait_recv()

    pltpu.make_async_copy(gbuf, dx_out, gsem.at[0]).wait()


def swap(value, third=0, second=0, group=0):
    pairs = []
    for t in range(2):
        for s in range(2):
            for g in range(2):
                pairs.append((t * 4 + s * 2 + g, (t ^ third) * 4 + (s ^ second) * 2 + (g ^ group)))
    return lax.ppermute(value, AXES, pairs)


def late_region(ref, color, f, q):
    if color == 0:
        return ref.at[pl.ds(pl.multiple_of(f * FB + q * PART[0], PART[0]), PART[0])]
    return ref.at[pl.ds(pl.multiple_of(q * PART[1], PART[1]), PART[1]), pl.ds(f * FB, FB)]


def my_quarter(color, flip_one, flip_core):
    a = lax.axis_index(('second', 'third')[color])
    g = lax.axis_index('group')
    return 2 * (1 - a if flip_one else a) + (1 - g if flip_core else g)


EARLY = 3 * FB
LEAD = 3
BUFS = {
    'a': ((3, EARLY, D), F32), 'b': ((3, D, EARLY), F32), 'ha': ((7, FB // 2, D), F32), 'hb': ((7, D // 2, FB), F32),
    'x': ((4, TOK // 4, D), BF16),
}


def block_jobs(b, out_o, out_i, sum_o, sum_i):
    jobs = []
    half_a = lax.axis_index('second') * (FB // 2)
    half_b = pl.ds(pl.multiple_of(lax.axis_index('third') * (D // 2), D // 2), D // 2)
    half_src = pl.ds(pl.multiple_of(b * D + lax.axis_index('third') * (D // 2), D // 2), D // 2)
    for f, count in RUNS[b]:
        width = count * FB
        rows = pl.ds(f * FB, width)
        jobs.append((out_o.at[pl.ds(b * FF + f * FB, width)], sum_o.at[rows], 'a', (pl.ds(0, width),)))
        jobs.append((out_i.at[pl.ds(b * D, D), rows], sum_i.at[:, rows], 'b', (slice(None), pl.ds(0, width))))
    for block, f in sum(GROUPS, ()):
        if block == b:
            cols = pl.ds(f * FB, FB)
            src = pl.multiple_of(b * FF + f * FB + half_a, FB // 2)
            dst = pl.multiple_of(f * FB + half_a, FB // 2)
            jobs.append((out_o.at[pl.ds(src, FB // 2)], sum_o.at[pl.ds(dst, FB // 2)], 'ha', ()))
            jobs.append((out_i.at[half_src, cols], sum_i.at[half_b, cols], 'hb', ()))
    return jobs


def late_jobs(group, late_a, late_b, out, flip_core):
    jobs = []
    for m, (b, f) in enumerate(GROUPS[group]):
        jobs.append((late_a.at[m], late_region(out[2 * b], 0, f, my_quarter(0, 1, flip_core))))
        jobs.append((late_b.at[m], late_region(out[2 * b + 1], 1, f, my_quarter(1, 1, flip_core))))
    return jobs


def run_moves(jobs, ready, bufs, isem, osem, rsem):
    direct = [pltpu.make_async_copy(src, dst, rsem.at[j]) for j, (src, dst) in enumerate(ready)]
    for copy in direct:
        copy.start()
    used, before, ins, outs = {}, [], [], []
    for j, (src, dst, kind, part) in enumerate(jobs):
        count = len(used.setdefault(kind, []))
        size = BUFS[kind][0][0]
        before.append(used[kind][count - size] if count >= size else None)
        used[kind].append(j)
        buf = bufs[kind].at[(count % size,) + part]
        ins.append(pltpu.make_async_copy(src, buf, isem.at[j]))
        outs.append(pltpu.make_async_copy(buf, dst, osem.at[j]))
    waited = set()
    for j in range(len(jobs) + LEAD if jobs else 0):
        if j < len(jobs):
            if before[j] is not None:
                outs[before[j]].wait()
                waited.add(before[j])
            ins[j].start()
        if j >= LEAD:
            ins[j - LEAD].wait()
            outs[j - LEAD].start()
    for j in range(len(jobs)):
        if j not in waited:
            outs[j].wait()
    for copy in direct:
        copy.wait()


def move(make_jobs, make_ready, kinds, counts, inputs, late, kept, new, flops):
    n_in, n_late, n_out = len(inputs), len(late), len(kept) + len(new)

    def body(*refs):
        outs = tuple(refs[n_in + n_late + len(kept):n_in + n_late + len(kept) + n_out])
        scratch = refs[n_in + n_late + len(kept) + n_out:]
        run_moves(make_jobs(refs[:n_in], outs), make_ready(refs[n_in:n_in + n_late], outs),
                  dict(zip(kinds, scratch)), *scratch[-3:])

    anywhere, onchip = pl.BlockSpec(memory_space=pl.ANY), pl.BlockSpec(memory_space=pltpu.VMEM)
    return pl.pallas_call(
        body,
        out_shape=tuple(jax.ShapeDtypeStruct(v.shape, v.dtype) for v in kept) + new,
        in_specs=[anywhere] * n_in + [onchip] * n_late + [anywhere] * len(kept),
        out_specs=[anywhere] * n_out,
        input_output_aliases={n_in + n_late + j: j for j in range(len(kept))},
        scratch_shapes=[pltpu.VMEM(*BUFS[kind]) for kind in kinds]
        + [pltpu.SemaphoreType.DMA((count,)) for count in (counts[0], counts[0], counts[1])],
        compiler_params=pltpu.CompilerParams(vmem_limit_bytes=(40 if kinds else 16) * 2 ** 20),
        cost_estimate=pl.CostEstimate(flops=flops, bytes_accessed=10 ** 6, transcendentals=0),
    )(*inputs, *late, *kept)


def solution(mesh):
    def device_step(x_one, z_one, x_two, z_two, grad_out, w1_in, w1_out, w2_in, w2_out):
        dma = pltpu.SemaphoreType.DMA
        late_shapes = []
        for group in GROUPS:
            late_shapes.append(jax.ShapeDtypeStruct((len(group), PART[0], D), F32))
            late_shapes.append(jax.ShapeDtypeStruct((len(group), PART[1], FB), F32))
        out_o, out_i, dx_tmp, *lates = pl.pallas_call(
            kernel,
            out_shape=(jax.ShapeDtypeStruct((2 * FF, D), F32), jax.ShapeDtypeStruct((2 * D, FF), F32),
                       jax.ShapeDtypeStruct((TOK, D), BF16),
                       *late_shapes),
            in_specs=[pl.BlockSpec(memory_space=pl.ANY)] * 9,
            out_specs=[pl.BlockSpec(memory_space=pl.ANY)] * 9,
            scratch_shapes=[
                pltpu.VMEM((TOK, D), BF16), pltpu.VMEM((TOK, D), BF16), pltpu.VMEM((TOK, D), F32),
                pltpu.VMEM((2, TOK, FB), BF16), pltpu.VMEM((2, FB, D), BF16), pltpu.VMEM((2, D, FB), BF16),
                pltpu.VMEM((D, FB), BF16), pltpu.VMEM((FB, D), BF16),
                pltpu.VMEM((FB, TOK), BF16), pltpu.VMEM((FB, TOK), BF16), pltpu.VMEM((2, TM, FB), BF16),
                pltpu.VMEM((NS, FB, D), BF16), pltpu.VMEM((NS, D, FB), BF16),
                pltpu.VMEM((R1, 3, PART[0], D), BF16), pltpu.VMEM((R1, 3, PART[1], FB), BF16),
                pltpu.VMEM((NP, PART[0], D), F32), pltpu.VMEM((NP, PART[1], FB), F32),
                pltpu.VMEM((R2, PART[0], D), F32), pltpu.VMEM((R2, PART[1], FB), F32),
                pltpu.VMEM((SD, PART[0], D), F32), pltpu.VMEM((SD, PART[1], FB), F32),
                dma((PIECES,)), dma, dma((2,)), dma((2,)), dma((2,)),
                dma((2, NS, 3)), dma((2, R1, 3)), dma((2, NP)), dma((2, R2)),
                dma((2, 2 * SD)), dma((2, SD, 2)), dma((2, RS, 2)), dma((2, RS)), dma((2, RS)),
            ],
            compiler_params=pltpu.CompilerParams(collective_id=0, has_side_effects=True,
                                                 vmem_limit_bytes=67043328),
        )(x_one, z_one, x_two, z_two, grad_out, w1_in, w1_out, w2_in, w2_out)
        def across(group):
            return swap(lates[2 * group], second=1), swap(lates[2 * group + 1], third=1)

        def to_pair(pair):
            return swap(pair[0], group=1), swap(pair[1], group=1)

        def none(i, o):
            return []

        x0, x1 = across(0), across(1)
        flat = (jax.ShapeDtypeStruct((FF, D), F32), jax.ShapeDtypeStruct((D, FF), F32))
        w2 = move(
            lambda i, o: block_jobs(0, i[0], i[1], o[0], o[1])
            + [(i[2].at[pl.ds(m * (TOK // 4), TOK // 4)], o[2].at[pl.ds(m * (TOK // 4), TOK // 4)], 'x', ()) for m in range(4)],
            none, ('a', 'b', 'ha', 'hb', 'x'), (20, 1), (out_o, out_i, dx_tmp), (), (),
            flat + (jax.ShapeDtypeStruct((TOK, D), BF16),), 2 * 10 ** 8)
        w2, x0, out_o, out_i, lates = lax.optimization_barrier((w2, x0, out_o, out_i, lates))
        x2 = across(2)
        f0 = to_pair(x0)
        sums = move(
            lambda i, o: block_jobs(1, i[0], i[1], o[2], o[3]),
            lambda v, o: late_jobs(0, v[0], v[1], o, 0),
            ('a', 'b', 'ha', 'hb'), (26, 8), (out_o, out_i), x0, w2[:2], flat, 2 * 10 ** 8)
        sums, x1 = lax.optimization_barrier((sums, x1))
        f1 = to_pair(x1)
        sums = move(none, lambda v, o: late_jobs(0, v[0], v[1], o, 1) + late_jobs(1, v[2], v[3], o, 0),
                    (), (1, 16), (), f0 + x1, sums, (), 10 ** 7)
        sums, x2 = lax.optimization_barrier((sums, x2))
        f2 = to_pair(x2)
        w1 = move(none, lambda v, o: late_jobs(1, v[0], v[1], (None, None) + o, 1) + late_jobs(2, v[2], v[3], (None, None) + o, 0),
                  (), (1, 14), (), f1 + x2, sums[2:], (), 10 ** 7)
        w1 = move(none, lambda v, o: late_jobs(2, v[0], v[1], (None, None) + o, 1),
                  (), (1, 6), (), f2, w1, (), 10 ** 7)
        return sums[0], sums[1], w1[0], w1[1], w2[2]

    row_spec = P(AXES, None)
    repl_spec = P()
    return jax.shard_map(
        device_step,
        mesh=mesh,
        in_specs=(row_spec, row_spec, row_spec, row_spec, row_spec, repl_spec, repl_spec, repl_spec, repl_spec),
        out_specs=(repl_spec, repl_spec, repl_spec, repl_spec, row_spec),
        check_vma=False,
    )
```

```python
import functools
import math
import jax
import jax.numpy as jnp
from jax import lax
from jax.experimental import pallas as pl
from jax.experimental.pallas import tpu as pltpu
from jax.sharding import PartitionSpec as P

AXES = ('third', 'second', 'group')
INV_ROOT_TWO = math.sqrt(0.5)
INV_ROOT_TWO_PI = 1.0 / math.sqrt(2.0 * math.pi)
MESH = pl.DeviceIdType.MESH
F32 = jnp.float32
BF16 = jnp.bfloat16
TOK, D, FF = 4096, 1024, 4096
FB = 256
NF = FF // FB
NC = 2 * NF
TM = 1024
PART = (FB // 4, D // 4)
COLS = (D, FB)
LB, LC, LD, LE = 1, 2, 4, 5
NS, NP = LB + 1, LC - LB + 1
R1, R2, SD, RS = 2 * LB + 3, 2 * (LC - LB) + 2, LE - LC + 1, 12
GROUPS = (((0, 3), (0, 7), (0, 11), (0, 15)), ((1, 3), (1, 5), (1, 7), (1, 9)), ((1, 11), (1, 14), (1, 15)))
RUNS = (((0, 3), (4, 3), (8, 3), (12, 3)),
        ((0, 3), (4, 1), (6, 1), (8, 1), (10, 1), (12, 2)))
PIECES = 4


def kernel(x1, z1, x2, z2, dy, w1i, w1o, w2i, w2o, out_o, out_i, dx_out,
           *rest):
    (late_a0, late_b0, late_a1, late_b1, late_a2, late_b2,
           gbuf, xbuf, acc, zbuf, wobuf, wibuf, wot, wit, ht, dzt, dzrow,
           slab_a, slab_b, got_a, got_b, part_a, part_b, swp_a, swp_b, sum_a, sum_b,
           gsem, xsem, zsem, wosem, wisem, s1, r1, s2, r2, lsem, s3, r3, sf, rf) = rest
    t, s, g = [lax.axis_index(k) for k in AXES]
    near_axis = (s, t)

    def peer(color, flip_one, flip_two, flip_core):
        ft, fs = (flip_two, flip_one) if color == 0 else (flip_one, flip_two)
        return (1 - t if ft else t, 1 - s if fs else s, 1 - g if flip_core else g)

    slab, got, part = (slab_a, slab_b), (got_a, got_b), (part_a, part_b)
    swp, sums = (swp_a, swp_b), (sum_a, sum_b)

    def quarter_of(color, flip_one, flip_core):
        a = near_axis[color]
        return 2 * (1 - a if flip_one else a) + (1 - g if flip_core else g)

    def slab_rows(color, q):
        return pl.ds(pl.multiple_of(q * PART[color], PART[color]), PART[color])

    def first(c, color, k):
        one, core = ((1, 0), (1, 1), (0, 1))[k]
        return pltpu.make_async_remote_copy(
            src_ref=slab[color].at[c % NS, slab_rows(color, quarter_of(color, one, core))],
            dst_ref=got[color].at[c % R1, k],
            send_sem=s1.at[color, c % NS, k], recv_sem=r1.at[color, c % R1, k],
            device_id=peer(color, one, 0, core), device_id_type=MESH)

    def second(c, color):
        return pltpu.make_async_remote_copy(
            src_ref=part[color].at[c % NP], dst_ref=swp[color].at[c % R2],
            send_sem=s2.at[color, c % NP], recv_sem=r2.at[color, c % R2],
            device_id=peer(color, 0, 1, 0), device_id_type=MESH)

    def region(c, color, q):
        b, f = c // NF, c % NF
        if color == 0:
            row = pl.multiple_of(b * FF + f * FB + q * PART[0], PART[0])
            return out_o.at[pl.ds(row, PART[0])]
        row = pl.multiple_of(b * D + q * PART[1], PART[1])
        return out_i.at[pl.ds(row, PART[1]), pl.ds(pl.multiple_of(f * FB, FB), FB)]

    def local(c, color):
        return pltpu.make_async_copy(sums[color].at[c % SD], region(c, color, quarter_of(color, 0, 0)),
                                     lsem.at[color, c % SD])

    lates = ((late_a0, late_b0), (late_a1, late_b1), (late_a2, late_b2))

    def is_late(c):
        odd = jnp.logical_and(c % 2 == 1, jnp.logical_or(c % 4 == 3, c >= NF + 4))
        return jnp.logical_and(jnp.logical_or(odd, c == NC - 2), c != NC - 3)

    def late_local(c, color, group):
        index = (c // 4, (c - NF - 3) // 2, jnp.where(c >= NC - 2, c - (NC - 3), 0))[group]
        return pltpu.make_async_copy(sums[color].at[c % SD], lates[group][color].at[index], lsem.at[color, SD + c % SD])

    def in_group(c, group):
        low, high = ((0, NF), (NF, NF + 10), (NF + 10, NC))[group]
        return jnp.logical_and(is_late(c), jnp.logical_and(c >= low, c < high))

    def third(c, color, k):
        return pltpu.make_async_remote_copy(
            src_ref=sums[color].at[c % SD], dst_ref=region(c, color, quarter_of(color, 0, 0)),
            send_sem=s3.at[color, c % SD, k], recv_sem=r3.at[color, c % RS, k],
            device_id=peer(color, 1 - k, 0, k), device_id_type=MESH)

    def forward(c, color):
        there = region(c, color, quarter_of(color, 1, 0))
        return pltpu.make_async_remote_copy(
            src_ref=there, dst_ref=there, send_sem=sf.at[color, c % RS], recv_sem=rf.at[color, c % RS],
            device_id=peer(color, 0, 0, 1), device_id_type=MESH)

    def loads(c, zr, wor, wir):
        f = c % NF
        cols = pl.ds(pl.multiple_of(f * FB, FB), FB)
        k = c % 2
        return (pltpu.make_async_copy(zr.at[:, cols], zbuf.at[k], zsem.at[k]),
                pltpu.make_async_copy(wor.at[cols], wobuf.at[k], wosem.at[k]),
                pltpu.make_async_copy(wir.at[:, cols], wibuf.at[k], wisem.at[k]))

    def start_loads(c):
        @pl.when(c < NF)
        def _():
            for copy in loads(c, z2, w2o, w2i):
                copy.start()

        @pl.when(jnp.logical_and(c >= NF, c < NC))
        def _():
            for copy in loads(c, z1, w1o, w1i):
                copy.start()

    start_loads(0)
    def first_rows(j):
        rows = pl.ds(j * (TOK // PIECES), TOK // PIECES)
        return pltpu.make_async_copy(dy.at[rows], gbuf.at[rows], gsem.at[j])

    for j in range(PIECES):
        first_rows(j).start()

    barrier = pltpu.get_barrier_semaphore()
    peers = ((0, 1, 0, 0), (0, 1, 0, 1), (1, 1, 0, 0), (1, 1, 0, 1), (0, 0, 0, 1))
    for who in peers:
        pl.semaphore_signal(barrier, inc=1, device_id=peer(*who), device_id_type=MESH)
    pl.semaphore_wait(barrier, len(peers))

    first_rows(0).wait()

    def compute_hidden(c):
        f = c % NF
        k = c % 2

        @pl.when(c == NF)
        def _():
            pltpu.make_async_copy(x1, xbuf, xsem).start()

        start_loads(c + 1)

        for copy in loads(c, z2, w2o, w2i):
            copy.wait()
        wot[...] = wobuf[k].T
        wit[...] = wibuf[k].T

        def grad_tile(r):
            rows = pl.ds(pl.multiple_of(r * TM, TM), TM)
            z_val = zbuf[k, rows, :].astype(F32)
            cdf_val = 0.5 * (1.0 + lax.erf(z_val * INV_ROOT_TWO))
            ht[:, rows] = (z_val * cdf_val).astype(BF16).T
            slope = cdf_val + z_val * jnp.exp(-0.5 * z_val * z_val) * INV_ROOT_TWO_PI
            grad_hidden = jnp.dot(gbuf[rows, :], wot[...], preferred_element_type=F32)
            grad_pre = (grad_hidden * slope).astype(BF16)
            dzt[:, rows] = grad_pre.T
            dzrow[r % 2] = grad_pre

        def add_tile(r, base):
            rows = pl.ds(pl.multiple_of(r * TM, TM), TM)
            acc[rows, :] = base[rows, :].astype(F32) + jnp.dot(dzrow[r % 2], wit[...], preferred_element_type=F32)

        def hidden_phase(base, before_rest):
            grad_tile(0)
            before_rest()

            @pl.loop(1, TOK // TM)
            def _(r):
                add_tile(r - 1, base)
                grad_tile(r)

            add_tile(TOK // TM - 1, base)

        @pl.when(f == 0)
        def _():
            def before_rest():
                @pl.when(c == 0)
                def _():
                    for j in range(1, PIECES):
                        first_rows(j).wait()
                    pltpu.make_async_copy(x2, xbuf, xsem).start()

            hidden_phase(gbuf, before_rest)

        @pl.when(f > 0)
        def _():
            hidden_phase(acc, lambda: None)

    def compute_weights(c):
        f = c % NF
        slab_a[c % NS] = jnp.dot(ht[...], gbuf[...], preferred_element_type=F32).astype(BF16)
        for j in range(3):
            first(c, 0, j).start()

        @pl.when(f == 0)
        def _():
            pltpu.make_async_copy(x2, xbuf, xsem).wait()

        slab_b[c % NS] = jnp.dot(dzt[...], xbuf[...], preferred_element_type=F32).T.astype(BF16)
        for j in range(3):
            first(c, 1, j).start()

        @pl.when(f == NF - 1)
        def _():
            @pl.loop(0, TOK // TM)
            def _(r):
                rows = pl.ds(pl.multiple_of(r * TM, TM), TM)
                gbuf[rows, :] = acc[rows, :].astype(BF16)

    def add_first(c):
        for color in range(2):
            for k in range(3):
                copy = first(c, color, k)
                copy.wait_recv()
                copy.wait_send()
            own = slab[color][c % NS, slab_rows(color, quarter_of(color, 0, 0)), :].astype(F32)
            near, far, pair = [got[color][c % R1, k].astype(F32) for k in range(3)]
            part[color][c % NP] = (own + pair) + (near + far)
            second(c, color).start()

    @pl.loop(0, NC + LE)
    def _(i):
        @pl.when(i < NC)
        def _():
            compute_hidden(i)

        @pl.when(i == 1)
        def _():
            add_first(0)

        @pl.when(i < NC)
        def _():
            compute_weights(i)

        @pl.when(i == NC - 1)
        def _():
            pltpu.make_async_copy(gbuf, dx_out, gsem.at[0]).start()

        @pl.when(jnp.logical_and(i >= 2, i < NC + LB))
        def _():
            add_first(i - LB)

        @pl.when(jnp.logical_and(jnp.logical_and(i >= 1, i != 2), i < NC + LC))
        def _():
            c = jnp.where(i == 1, 0, i - LC)
            for color in range(2):
                copy = second(c, color)
                copy.wait_recv()
                copy.wait_send()
                sums[color][c % SD] = part[color][c % NP] + swp[color][c % R2]
            for color in range(2):
                third(c, color, 1).start()
                local(c, color).start()

            @pl.when(jnp.logical_not(is_late(c)))
            def _():
                for color in range(2):
                    third(c, color, 0).start()

            for group in range(len(GROUPS)):
                @pl.when(in_group(c, group))
                def _():
                    for color in range(2):
                        late_local(c, color, group).start()

        @pl.when(jnp.logical_and(jnp.logical_and(i >= LD, i < NC + LD), jnp.logical_not(is_late(i - LD))))
        def _():
            c = i - LD
            for color in range(2):
                third(c, color, 0).wait_recv()
                forward(c, color).start()

        @pl.when(jnp.logical_and(i >= LE, i < NC + LE))
        def _():
            c = i - LE
            for color in range(2):
                third(c, color, 1).wait_recv()
                third(c, color, 1).wait_send()
                local(c, color).wait()

            @pl.when(is_late(c))
            def _():
                for color in range(2):
                    pltpu.make_async_copy(sums[color].at[c % SD], lates[0][color].at[0],
                                          lsem.at[color, SD + c % SD]).wait()

            @pl.when(jnp.logical_not(is_late(c)))
            def _():
                for color in range(2):
                    third(c, color, 0).wait_send()
                    forward(c, color).wait_send()
                    forward(c, color).wait_recv()

    pltpu.make_async_copy(gbuf, dx_out, gsem.at[0]).wait()


def swap(value, third=0, second=0, group=0):
    pairs = []
    for t in range(2):
        for s in range(2):
            for g in range(2):
                pairs.append((t * 4 + s * 2 + g, (t ^ third) * 4 + (s ^ second) * 2 + (g ^ group)))
    return lax.ppermute(value, AXES, pairs)


def late_region(ref, color, f, q):
    if color == 0:
        return ref.at[pl.ds(pl.multiple_of(f * FB + q * PART[0], PART[0]), PART[0])]
    return ref.at[pl.ds(pl.multiple_of(q * PART[1], PART[1]), PART[1]), pl.ds(f * FB, FB)]


def my_quarter(color, flip_one, flip_core):
    a = lax.axis_index(('second', 'third')[color])
    g = lax.axis_index('group')
    return 2 * (1 - a if flip_one else a) + (1 - g if flip_core else g)


EARLY = 3 * FB
LEAD = 3
BUFS = {
    'a': ((3, EARLY, D), F32), 'b': ((3, D, EARLY), F32), 'ha': ((7, FB // 2, D), F32), 'hb': ((7, D // 2, FB), F32),
    'x': ((4, TOK // 4, D), BF16),
}


def block_jobs(b, out_o, out_i, sum_o, sum_i):
    jobs = []
    half_a = lax.axis_index('second') * (FB // 2)
    half_b = pl.ds(pl.multiple_of(lax.axis_index('third') * (D // 2), D // 2), D // 2)
    half_src = pl.ds(pl.multiple_of(b * D + lax.axis_index('third') * (D // 2), D // 2), D // 2)
    for f, count in RUNS[b]:
        width = count * FB
        rows = pl.ds(f * FB, width)
        jobs.append((out_o.at[pl.ds(b * FF + f * FB, width)], sum_o.at[rows], 'a', (pl.ds(0, width),)))
        jobs.append((out_i.at[pl.ds(b * D, D), rows], sum_i.at[:, rows], 'b', (slice(None), pl.ds(0, width))))
    for block, f in sum(GROUPS, ()):
        if block == b:
            cols = pl.ds(f * FB, FB)
            src = pl.multiple_of(b * FF + f * FB + half_a, FB // 2)
            dst = pl.multiple_of(f * FB + half_a, FB // 2)
            jobs.append((out_o.at[pl.ds(src, FB // 2)], sum_o.at[pl.ds(dst, FB // 2)], 'ha', ()))
            jobs.append((out_i.at[half_src, cols], sum_i.at[half_b, cols], 'hb', ()))
    return jobs


def late_jobs(group, late_a, late_b, out, flip_core):
    jobs = []
    for m, (b, f) in enumerate(GROUPS[group]):
        jobs.append((late_a.at[m], late_region(out[2 * b], 0, f, my_quarter(0, 1, flip_core))))
        jobs.append((late_b.at[m], late_region(out[2 * b + 1], 1, f, my_quarter(1, 1, flip_core))))
    return jobs


def run_moves(jobs, ready, bufs, isem, osem, rsem):
    direct = [pltpu.make_async_copy(src, dst, rsem.at[j]) for j, (src, dst) in enumerate(ready)]
    for copy in direct:
        copy.start()
    used, before, ins, outs = {}, [], [], []
    for j, (src, dst, kind, part) in enumerate(jobs):
        count = len(used.setdefault(kind, []))
        size = BUFS[kind][0][0]
        before.append(used[kind][count - size] if count >= size else None)
        used[kind].append(j)
        buf = bufs[kind].at[(count % size,) + part]
        ins.append(pltpu.make_async_copy(src, buf, isem.at[j]))
        outs.append(pltpu.make_async_copy(buf, dst, osem.at[j]))
    waited = set()
    for j in range(len(jobs) + LEAD if jobs else 0):
        if j < len(jobs):
            if before[j] is not None:
                outs[before[j]].wait()
                waited.add(before[j])
            ins[j].start()
        if j >= LEAD:
            ins[j - LEAD].wait()
            outs[j - LEAD].start()
    for j in range(len(jobs)):
        if j not in waited:
            outs[j].wait()
    for copy in direct:
        copy.wait()


def move(make_jobs, make_ready, kinds, counts, inputs, late, kept, new, flops):
    n_in, n_late, n_out = len(inputs), len(late), len(kept) + len(new)

    def body(*refs):
        outs = tuple(refs[n_in + n_late + len(kept):n_in + n_late + len(kept) + n_out])
        scratch = refs[n_in + n_late + len(kept) + n_out:]
        run_moves(make_jobs(refs[:n_in], outs), make_ready(refs[n_in:n_in + n_late], outs),
                  dict(zip(kinds, scratch)), *scratch[-3:])

    anywhere, onchip = pl.BlockSpec(memory_space=pl.ANY), pl.BlockSpec(memory_space=pltpu.VMEM)
    return pl.pallas_call(
        body,
        out_shape=tuple(jax.ShapeDtypeStruct(v.shape, v.dtype) for v in kept) + new,
        in_specs=[anywhere] * n_in + [onchip] * n_late + [anywhere] * len(kept),
        out_specs=[anywhere] * n_out,
        input_output_aliases={n_in + n_late + j: j for j in range(len(kept))},
        scratch_shapes=[pltpu.VMEM(*BUFS[kind]) for kind in kinds]
        + [pltpu.SemaphoreType.DMA((count,)) for count in (counts[0], counts[0], counts[1])],
        compiler_params=pltpu.CompilerParams(vmem_limit_bytes=(40 if kinds else 16) * 2 ** 20),
        cost_estimate=pl.CostEstimate(flops=flops, bytes_accessed=10 ** 6, transcendentals=0),
    )(*inputs, *late, *kept)


def solution(mesh):
    def device_step(x_one, z_one, x_two, z_two, grad_out, w1_in, w1_out, w2_in, w2_out):
        dma = pltpu.SemaphoreType.DMA
        late_shapes = []
        for group in GROUPS:
            late_shapes.append(jax.ShapeDtypeStruct((len(group), PART[0], D), F32))
            late_shapes.append(jax.ShapeDtypeStruct((len(group), PART[1], FB), F32))
        out_o, out_i, dx_tmp, *lates = pl.pallas_call(
            kernel,
            out_shape=(jax.ShapeDtypeStruct((2 * FF, D), F32), jax.ShapeDtypeStruct((2 * D, FF), F32),
                       jax.ShapeDtypeStruct((TOK, D), BF16),
                       *late_shapes),
            in_specs=[pl.BlockSpec(memory_space=pl.ANY)] * 9,
            out_specs=[pl.BlockSpec(memory_space=pl.ANY)] * 9,
            scratch_shapes=[
                pltpu.VMEM((TOK, D), BF16), pltpu.VMEM((TOK, D), BF16), pltpu.VMEM((TOK, D), F32),
                pltpu.VMEM((2, TOK, FB), BF16), pltpu.VMEM((2, FB, D), BF16), pltpu.VMEM((2, D, FB), BF16),
                pltpu.VMEM((D, FB), BF16), pltpu.VMEM((FB, D), BF16),
                pltpu.VMEM((FB, TOK), BF16), pltpu.VMEM((FB, TOK), BF16), pltpu.VMEM((2, TM, FB), BF16),
                pltpu.VMEM((NS, FB, D), BF16), pltpu.VMEM((NS, D, FB), BF16),
                pltpu.VMEM((R1, 3, PART[0], D), BF16), pltpu.VMEM((R1, 3, PART[1], FB), BF16),
                pltpu.VMEM((NP, PART[0], D), F32), pltpu.VMEM((NP, PART[1], FB), F32),
                pltpu.VMEM((R2, PART[0], D), F32), pltpu.VMEM((R2, PART[1], FB), F32),
                pltpu.VMEM((SD, PART[0], D), F32), pltpu.VMEM((SD, PART[1], FB), F32),
                dma((PIECES,)), dma, dma((2,)), dma((2,)), dma((2,)),
                dma((2, NS, 3)), dma((2, R1, 3)), dma((2, NP)), dma((2, R2)),
                dma((2, 2 * SD)), dma((2, SD, 2)), dma((2, RS, 2)), dma((2, RS)), dma((2, RS)),
            ],
            compiler_params=pltpu.CompilerParams(collective_id=0, has_side_effects=True,
                                                 vmem_limit_bytes=67043328),
        )(x_one, z_one, x_two, z_two, grad_out, w1_in, w1_out, w2_in, w2_out)
        def across(group):
            return swap(lates[2 * group], second=1), swap(lates[2 * group + 1], third=1)

        def to_pair(pair):
            return swap(pair[0], group=1), swap(pair[1], group=1)

        def none(i, o):
            return []

        x0, x1 = across(0), across(1)
        flat = (jax.ShapeDtypeStruct((FF, D), F32), jax.ShapeDtypeStruct((D, FF), F32))
        w2 = move(
            lambda i, o: block_jobs(0, i[0], i[1], o[0], o[1])
            + [(i[2].at[pl.ds(m * (TOK // 4), TOK // 4)], o[2].at[pl.ds(m * (TOK // 4), TOK // 4)], 'x', ()) for m in range(4)],
            none, ('a', 'b', 'ha', 'hb', 'x'), (20, 1), (out_o, out_i, dx_tmp), (), (),
            flat + (jax.ShapeDtypeStruct((TOK, D), BF16),), 2 * 10 ** 8)
        w2, x0, out_o, out_i, lates = lax.optimization_barrier((w2, x0, out_o, out_i, lates))
        x2 = across(2)
        f0 = to_pair(x0)
        sums = move(
            lambda i, o: block_jobs(1, i[0], i[1], o[2], o[3]),
            lambda v, o: late_jobs(0, v[0], v[1], o, 0),
            ('a', 'b', 'ha', 'hb'), (26, 8), (out_o, out_i), x0, w2[:2], flat, 2 * 10 ** 8)
        sums, x1 = lax.optimization_barrier((sums, x1))
        f1 = to_pair(x1)
        sums = move(none, lambda v, o: late_jobs(0, v[0], v[1], o, 1) + late_jobs(1, v[2], v[3], o, 0),
                    (), (1, 16), (), f0 + x1, sums, (), 10 ** 7)
        sums, x2 = lax.optimization_barrier((sums, x2))
        f2 = to_pair(x2)
        w1 = move(none, lambda v, o: late_jobs(1, v[0], v[1], (None, None) + o, 1) + late_jobs(2, v[2], v[3], (None, None) + o, 0),
                  (), (1, 14), (), f1 + x2, sums[2:], (), 10 ** 7)
        w1 = move(none, lambda v, o: late_jobs(2, v[0], v[1], (None, None) + o, 1),
                  (), (1, 6), (), f2, w1, (), 10 ** 7)
        return sums[0], sums[1], w1[0], w1[1], w2[2]

    row_spec = P(AXES, None)
    repl_spec = P()
    return jax.shard_map(
        device_step,
        mesh=mesh,
        in_specs=(row_spec, row_spec, row_spec, row_spec, row_spec, repl_spec, repl_spec, repl_spec, repl_spec),
        out_specs=(repl_spec, repl_spec, repl_spec, repl_spec, row_spec),
        check_vma=False,
    )
```
